32 devices in a mesh: grp: 8 (over z, y), slab: 4 (over x, core).
Axes of the slice: x: 2, y: 2, z: 4, core: 2. Of those that a mesh axis runs over, the one named last changes fastest.
Arguments:
- grids: float32 [8, 512, 4096], P('grp', 'slab'), may hold values from -6 to 6
- first_level: int32 [8], P('grp'), may hold values from 6 to 8, as said below
- coeffs: int32 [8], P('grp'), may hold values from -3 to 3
- slot_map: int32 [8, 512], P('grp', 'slab'), may hold values from 0 to 1023, as said below
Outputs:
- combined_grid: float32 [8, 512, 4096], P('grp', 'slab')
The draws below stay inside these ranges and needn't reach their ends.
Inputs may be any that keep to these rules, and one draw needn't show every extreme that they name: The second dimension of grid g has level 9 minus first_level[g]. Every value of the range is taken by some grid. `slot_map`: grid g's point with first coordinate i of 2^a points lies at position i / 2^a of a periodic unit interval, and likewise in the second dimension. Two rows of any grids at the same position in the first two dimensions share a slot; rows of one grid have distinct slots; every slot is used by some grid. The rows held by the s-th index of slab (first coordinates in the s-th of 4 equal ranges) of every grid have slots in the s-th of 4 equal aligned ranges of the 1024 slots.
All inputs are finite; a program needn't handle non-finite values.
Results may differ from the reference program's by a relative error of at most 0.0003.
Values sent between devices are 32-bit elements; how exact they have to be, the bound alone decides.
A program may use at most 64 MiB of HBM per device.

```python
import jax
import jax.numpy as jnp
from jax import lax

P2 = 16
P3 = 16
P4 = 16
LEVEL_SUM = 9
GROUPS = 8
ROWS = 512
INNER = 4096
N_SLAB = 4


def level_draw(key):
    order = jax.random.permutation(jax.random.fold_in(key, 11), GROUPS)
    return (LEVEL_SUM - 3 + order % 3).astype(jnp.int32)


def draw_first_level(key, part):
    return level_draw(key)


def draw_slot_map(key, part):
    first = level_draw(key)[:, None]
    second = LEVEL_SUM - first
    row_ids = jnp.arange(ROWS, dtype=jnp.int32)[None, :]
    along_first = row_ids >> second
    along_second = row_ids & (1 << second) - 1
    rev_first = jnp.zeros((GROUPS, ROWS), jnp.int32)
    rev_second = jnp.zeros((GROUPS, ROWS), jnp.int32)
    for place in range(LEVEL_SUM):
        up_first = jnp.maximum(first - 1 - place, 0)
        up_second = jnp.maximum(second - 1 - place, 0)
        rev_first = rev_first + jnp.where(place < first, (along_first >> place & 1) << up_first, 0)
        rev_second = rev_second + jnp.where(place < second, (along_second >> place & 1) << up_second, 0)
    slab_of = along_first * N_SLAB >> first
    coarse = rev_first // N_SLAB
    per_slab = 2 * ROWS // N_SLAB
    band_one = ROWS // N_SLAB
    band_two = band_one + ROWS // (2 * N_SLAB)
    rank = jnp.where(rev_second < 2, coarse * 2 + rev_second, jnp.where(rev_second < 4, band_one + coarse * 2 + rev_second - 2, band_two + coarse * 4 + rev_second - 4))
    keys = jax.random.split(jax.random.fold_in(key, 23), N_SLAB)
    shuffles = jax.vmap(lambda single: jax.random.permutation(single, per_slab))(keys)
    return (slab_of * per_slab + shuffles[slab_of, rank]).astype(jnp.int32)


def set_ends(entries, own_key, least, high):
    longest = entries.shape.index(max(entries.shape))
    spots = []
    for shift in (0, 1):
        where = [jax.random.randint(jax.random.fold_in(own_key, axis), (), 0, length) for axis, length in enumerate(entries.shape)]
        where[longest] = (where[longest] + shift) % entries.shape[longest]
        spots.append(tuple(where))
    return entries.at[spots[0]].set(least).at[spots[1]].set(high)


def level_of(stream_key, extent, cuts, smallest, top_value):
    def one(axis_at, parts):
        heights = jax.random.uniform(jax.random.fold_in(jax.random.fold_in(stream_key, 6), axis_at), (parts,), jnp.float32, smallest / len(cuts), top_value / len(cuts))
        return jnp.repeat(jnp.exp(heights), extent[axis_at] // parts).reshape((-1,) + (1,) * (len(extent) - axis_at - 1))

    loudness = one(*cuts[0])
    for cut in cuts[1:]:
        loudness = loudness * one(*cut)
    return loudness


def noise(key, extent, scale, limit, pieces=(), held_as=jnp.bfloat16):
    level = level_of(key, extent, pieces, -0.22, 0.18) if pieces else 1.0
    result = jax.random.normal(key, extent, jnp.float32) * scale * level
    return jnp.minimum(jnp.maximum(result, -limit), limit).astype(held_as)


def setup_inputs(seed: int = 0) -> dict:
    seeds = jax.random.split(jax.random.key(seed), 5)
    grids = noise(seeds[0], (GROUPS, ROWS, INNER), 1.0, 6.0, ((0, 8), (1, 4)), jnp.float32)
    first_level = draw_first_level(jax.random.fold_in(seeds[4], 71), 0)
    coeffs = set_ends(jax.random.randint(seeds[2], (GROUPS,), -3, 4), jax.random.fold_in(seeds[2], 1), -3, 3).astype(jnp.int32)
    slot_map = draw_slot_map(jax.random.fold_in(seeds[4], 71), 0)
    return dict(grids=grids, first_level=first_level, coeffs=coeffs, slot_map=slot_map)


def hier_weight(target, source, period):
    spread = target & (-target)
    interior = (target != 0).astype(jnp.float32)
    left_side = (source == target - spread).astype(jnp.float32)
    right_side = (source == (target + spread) % period).astype(jnp.float32)
    return (target == source).astype(jnp.float32) - 0.5 * interior * (left_side + right_side)


def dehier_weight(target, source, period):
    spread = jnp.maximum(source & (-source), 1).astype(jnp.float32)
    apart = jnp.abs(target - source)
    apart = jnp.minimum(apart, period - apart).astype(jnp.float32)
    return jnp.where(source == 0, 1.0, jnp.maximum(0.0, 1.0 - apart / spread))


def square_table(maker, length):
    points = jnp.arange(length, dtype=jnp.int32)
    return maker(points[:, None], points[None, :], length)


def inner_apply(values, third_op, rest_op):
    count = values.shape[0]
    shaped = values.reshape(count, P2, P3 * P4)
    shaped = jnp.einsum("ij,rjk->rik", third_op, shaped, precision=lax.Precision.HIGHEST)
    shaped = jnp.einsum("rjk,lk->rjl", shaped, rest_op, precision=lax.Precision.HIGHEST)
    return shaped.reshape(count, P2 * P3 * P4)


def row_matrix(maker, level):
    second = LEVEL_SUM - level
    row_ids = jnp.arange(ROWS, dtype=jnp.int32)
    first_pos = row_ids >> second
    second_pos = row_ids & ((1 << second) - 1)
    first_part = maker(first_pos[:, None], first_pos[None, :], 1 << level)
    second_part = maker(second_pos[:, None], second_pos[None, :], 1 << second)
    return first_part * second_part


def reference(grids, first_level, coeffs, slot_map):
    hier_third = square_table(hier_weight, P2)
    hier_rest = jnp.kron(square_table(hier_weight, P3), square_table(hier_weight, P4))
    back_third = square_table(dehier_weight, P2)
    back_rest = jnp.kron(square_table(dehier_weight, P3), square_table(dehier_weight, P4))

    def add_group(table, item):
        grid, level, factor, slots = item
        mixed = jnp.dot(row_matrix(hier_weight, level), grid, precision=lax.Precision.HIGHEST, preferred_element_type=jnp.float32)
        surplus = inner_apply(mixed, hier_third, hier_rest)
        return table.at[slots].add(factor.astype(jnp.float32) * surplus), None

    table, unused = lax.scan(add_group, jnp.zeros((2 * ROWS, P2 * P3 * P4), jnp.float32), (grids, first_level, coeffs, slot_map))

    def rebuild(item):
        level, slots = item
        values = table[slots]
        nodal = jnp.dot(row_matrix(dehier_weight, level), values, precision=lax.Precision.HIGHEST, preferred_element_type=jnp.float32)
        return inner_apply(nodal, back_third, back_rest)

    return lax.map(rebuild, (first_level, slot_map))
```

```python
import functools

import jax
import jax.numpy as jnp
from jax import lax
from jax.experimental import pallas as pl
from jax.experimental.pallas import tpu as pltpu
from jax.sharding import PartitionSpec as P

P2 = 16
P3 = 16
P4 = 16
LEVEL_SUM = 9
PLANE = 8
ROWS = 512
MESH = pl.DeviceIdType.MESH


def hier_weight(target, source, period):
    spread = target & -target
    interior = (target != 0).astype(jnp.float32)
    left_side = (source == target - spread).astype(jnp.float32)
    right_side = (source == (target + spread) % period).astype(jnp.float32)
    return (target == source).astype(jnp.float32) - 0.5 * interior * (left_side + right_side)


def dehier_weight(target, source, period):
    spread = jnp.maximum(source & -source, 1).astype(jnp.float32)
    apart = jnp.abs(target - source)
    apart = jnp.minimum(apart, period - apart).astype(jnp.float32)
    return jnp.where(source == 0, 1.0, jnp.maximum(0.0, 1.0 - apart / spread))


def square_table(maker, length):
    points = jnp.arange(length, dtype=jnp.int32)
    return maker(points[:, None], points[None, :], length)


def inner_apply(values, third_op, rest_op):
    count = values.shape[0]
    shaped = values.reshape(count, P2, P3 * P4)
    shaped = jnp.einsum("ij,rjk->rik", third_op, shaped, precision=lax.Precision.HIGHEST)
    shaped = jnp.einsum("rjk,lk->rjl", shaped, rest_op, precision=lax.Precision.HIGHEST)
    return shaped.reshape(count, P2 * P3 * P4)


def exact_dot(left, right):
    return jnp.dot(left, right, precision=lax.Precision.HIGHEST, preferred_element_type=jnp.float32)


def shards(grids, first_level, coeffs, slot_map):
    grid_rows = grids[0]
    level = first_level[0]
    second = LEVEL_SUM - level
    rows_dev = grid_rows.shape[0]
    width = grid_rows.shape[1]
    slabs = lax.axis_size("slab")
    slab_index = lax.axis_index("slab")
    span = rows_dev >> second
    row_ids = jnp.arange(rows_dev, dtype=jnp.int32)
    first_pos = row_ids >> second
    second_pos = row_ids & (1 << second) - 1
    slab_ids = jnp.arange(slabs, dtype=jnp.int32)
    same_first = (first_pos[:, None] == first_pos[None, :]).astype(jnp.float32)
    hier_third = square_table(hier_weight, P2)
    hier_rest = jnp.kron(square_table(hier_weight, P3), square_table(hier_weight, P4))
    values = inner_apply(grid_rows, hier_third, hier_rest)
    second_op = same_first * hier_weight(second_pos[:, None], second_pos[None, :], 1 << second)
    values = exact_dot(second_op, values)
    plane = values[:PLANE]
    planes = lax.all_gather(plane[None], "slab", axis=0, tiled=True)
    following = lax.dynamic_index_in_dim(planes, (slab_index + 1) % slabs, 0, keepdims=False)
    extended = jnp.concatenate([values, following], axis=0)
    ext_ids = jnp.arange(rows_dev + PLANE, dtype=jnp.int32)
    ext_first = ext_ids >> second
    ext_second = ext_ids & (1 << second) - 1
    spread = first_pos & -first_pos
    interior = (first_pos != 0).astype(jnp.float32)[:, None]
    same_second = (second_pos[:, None] == ext_second[None, :]).astype(jnp.float32)
    centre = (ext_first[None, :] == first_pos[:, None]).astype(jnp.float32)
    below = (ext_first[None, :] == (first_pos - spread)[:, None]).astype(jnp.float32)
    above = (ext_first[None, :] == (first_pos + spread)[:, None]).astype(jnp.float32)
    fine_op = same_second * (centre - 0.5 * interior * (below + above))
    surplus = exact_dot(fine_op, extended)
    coarse_weights = hier_weight(slab_index, slab_ids, slabs)
    coarse = jnp.einsum("q,qpk->pk", coarse_weights, planes, precision=lax.Precision.HIGHEST)
    padded = jnp.concatenate([coarse, jnp.zeros((rows_dev - PLANE, width), jnp.float32)], axis=0)
    surplus = jnp.where((first_pos == 0)[:, None], padded, surplus)
    scaled = coeffs[0].astype(jnp.float32) * surplus
    per_slab = 2 * ROWS // slabs
    slot_local = slot_map[0] % per_slab
    slot_ids = jnp.arange(per_slab, dtype=jnp.int32)
    gather_op = (slot_local[None, :] == slot_ids[:, None]).astype(jnp.float32)
    term = exact_dot(gather_op, scaled)
    total = lax.psum(term, "grp")
    spread_op = (slot_local[:, None] == slot_ids[None, :]).astype(jnp.float32)
    combined = exact_dot(spread_op, total)
    back_third = square_table(dehier_weight, P2)
    back_rest = jnp.kron(square_table(dehier_weight, P3), square_table(dehier_weight, P4))
    values = inner_apply(combined, back_third, back_rest)
    back_second = same_first * dehier_weight(second_pos[:, None], second_pos[None, :], 1 << second)
    values = exact_dot(back_second, values)
    top_plane = values[:PLANE]
    top_planes = lax.all_gather(top_plane[None], "slab", axis=0, tiled=True)
    here_weights = dehier_weight(slab_index, slab_ids, slabs)
    there_weights = dehier_weight((slab_index + 1) % slabs, slab_ids, slabs)
    here = jnp.einsum("q,qpk->pk", here_weights, top_planes, precision=lax.Precision.HIGHEST)
    there = jnp.einsum("q,qpk->pk", there_weights, top_planes, precision=lax.Precision.HIGHEST)
    same_row_second = (second_pos[:, None] == second_pos[None, :]).astype(jnp.float32)
    inside = (first_pos[None, :] != 0).astype(jnp.float32)
    local_op = (
        same_row_second * inside * dehier_weight(first_pos[:, None], first_pos[None, :], 2 * span)
    )
    fraction = first_pos.astype(jnp.float32) / span.astype(jnp.float32)
    plane_ids = jnp.arange(PLANE, dtype=jnp.int32)
    plane_pick = (second_pos[:, None] == plane_ids[None, :]).astype(jnp.float32)
    nodal = exact_dot(local_op, values)
    nodal = nodal + exact_dot((1.0 - fraction)[:, None] * plane_pick, here)
    nodal = nodal + exact_dot(fraction[:, None] * plane_pick, there)
    return nodal[None]


HALVES = 2
LANES = 128


def split_pair(values):
    high = values.astype(jnp.bfloat16)
    low = (values - high.astype(jnp.float32)).astype(jnp.bfloat16)
    return high, low


def mix(weights, body, edge):
    body_high, body_low = split_pair(body)
    edge_high, edge_low = split_pair(edge)
    stacked = jnp.concatenate([body_high, body_low, edge_high, edge_low], axis=0)
    return jnp.dot(weights, stacked, preferred_element_type=jnp.float32)


def kernel(groups, slabs, per_slab, grid_ref, slot_ref, fwd_ref, back_ref, out_ref,
           sent, got, table, spread, back, vals, planes, tops, slots, pick, place,
           plane_send, plane_recv, slot_send, slot_recv, fwd_send, fwd_recv,
           back_send, back_recv, top_send, top_recv):
    me = lax.axis_index("grp")
    here = lax.axis_index("slab")
    rows = grid_ref.shape[0]
    piece = sent.shape[3]
    chunk = HALVES * piece

    def group_at(step):
        return lax.rem(me + step, groups)

    def slab_at(step):
        return lax.rem(here + step, slabs)

    def columns(owner, half):
        return pl.ds(pl.multiple_of(owner * chunk + half * piece, piece), piece)

    barrier = pltpu.get_barrier_semaphore()
    for step in range(1, groups):
        pl.semaphore_signal(barrier, inc=1, device_id={"grp": group_at(step)}, device_id_type=MESH)
    for step in range(1, slabs):
        pl.semaphore_signal(barrier, inc=1, device_id={"slab": slab_at(step)}, device_id_type=MESH)
    pl.semaphore_wait(barrier, groups + slabs - 2)

    order = list(range(1, groups)) + [0]
    pending = []

    def plane_copy(half, step, away):
        cols = columns(group_at(step), half)
        return pltpu.make_async_remote_copy(
            src_ref=grid_ref.at[pl.ds(0, PLANE), cols],
            dst_ref=planes.at[away, :, cols],
            send_sem=plane_send.at[half, step, away],
            recv_sem=plane_recv.at[half, step, away],
            device_id={"slab": slab_at(away)},
            device_id_type=MESH,
        )

    def slot_copy(step):
        return pltpu.make_async_remote_copy(
            src_ref=slot_ref,
            dst_ref=slots.at[step],
            send_sem=slot_send.at[step],
            recv_sem=slot_recv.at[step],
            device_id={"grp": group_at(step)},
            device_id_type=MESH,
        )

    def fwd_copy(half, step):
        return pltpu.make_async_remote_copy(
            src_ref=sent.at[half, step],
            dst_ref=got.at[half, step],
            send_sem=fwd_send.at[half, step],
            recv_sem=fwd_recv.at[half, step],
            device_id={"grp": group_at(step)},
            device_id_type=MESH,
        )

    def back_copy(half, step):
        return pltpu.make_async_remote_copy(
            src_ref=back.at[half, step],
            dst_ref=vals.at[half, step],
            send_sem=back_send.at[half, step],
            recv_sem=back_recv.at[half, step],
            device_id={"grp": lax.rem(me + groups - step, groups)},
            device_id_type=MESH,
        )

    def top_copy(half, step, away):
        return pltpu.make_async_remote_copy(
            src_ref=vals.at[half, step, pl.ds(0, PLANE), :],
            dst_ref=tops.at[half, step, away],
            send_sem=top_send.at[half, step, away],
            recv_sem=top_recv.at[half, step, away],
            device_id={"slab": slab_at(away)},
            device_id_type=MESH,
        )

    for half in range(HALVES):
        for step in order:
            for away in range(1, slabs):
                copy = plane_copy(half, step, away)
                copy.start()
                pending.append(copy)
    for step in range(1, groups):
        copy = slot_copy(step)
        copy.start()
        pending.append(copy)

    fwd_weights = fwd_ref[...]
    for half in range(HALVES):
        for step in order:
            for away in range(1, slabs):
                plane_copy(half, step, away).wait_recv()
            cols = columns(group_at(step), half)
            edge = [planes[away, :, cols] for away in range(1, slabs)]
            edge.append(jnp.zeros((PLANE, piece), jnp.float32))
            scaled = mix(fwd_weights, grid_ref[:, cols], jnp.concatenate(edge, axis=0))
            if step:
                sent[half, step] = scaled
                copy = fwd_copy(half, step)
                copy.start()
                pending.append(copy)
            else:
                got[half, step] = scaled

    slot_ids = lax.broadcasted_iota(jnp.int32, (per_slab, rows), 0)
    for step in [0] + order[:-1]:
        if step:
            slot_copy(step).wait_recv()
            row_slots = slots[step, 0:1, :]
        else:
            row_slots = slot_ref[0:1, :]
        hit = jnp.where(slot_ids == row_slots, 1.0, 0.0)
        flat = hit.astype(jnp.bfloat16)
        pick[step] = jnp.concatenate([flat, flat], axis=1)
        turned = jnp.transpose(hit).astype(jnp.bfloat16)
        place[step] = jnp.concatenate([turned, turned], axis=1)

    for half in range(HALVES):
        for count, step in enumerate([0] + order[:-1]):
            if step:
                fwd_copy(half, step).wait_recv()
            high, low = split_pair(got[half, step])
            term = jnp.dot(pick[step], jnp.concatenate([high, low], axis=0), preferred_element_type=jnp.float32)
            table[...] = term if count == 0 else table[...] + term
        high, low = split_pair(table[...])
        spread[...] = jnp.concatenate([high, low], axis=0)
        for step in order:
            rebuilt = jnp.dot(place[step], spread[...], preferred_element_type=jnp.float32)
            if step:
                back[half, step] = rebuilt
                copy = back_copy(half, step)
                copy.start()
                pending.append(copy)
            else:
                vals[half, step] = rebuilt

    back_weights = back_ref[...]

    def finish(half, step):
        for away in range(1, slabs):
            top_copy(half, step, away).wait_recv()
        edge = [tops[half, step, away] for away in range(1, slabs)]
        edge.append(jnp.zeros((PLANE, piece), jnp.float32))
        out_ref[:, columns(group_at(step), half)] = mix(back_weights, vals[half, step], jnp.concatenate(edge, axis=0))

    waiting = []
    for half in range(HALVES):
        for step in [0] + order[:-1]:
            if step:
                back_copy(half, step).wait_recv()
            for away in range(1, slabs):
                copy = top_copy(half, step, away)
                copy.start()
                pending.append(copy)
            waiting.append((half, step))
            if len(waiting) > 3:
                finish(*waiting.pop(0))
    for item in waiting:
        finish(*item)
    for copy in pending:
        copy.wait_send()


def fused_shards(grids, first_level, coeffs, slot_map):
    grid_rows = grids[0]
    level = first_level[0]
    second = LEVEL_SUM - level
    rows_dev, width = grid_rows.shape
    slabs = lax.axis_size("slab")
    groups = lax.axis_size("grp")
    here = lax.axis_index("slab")
    per_slab = 2 * ROWS // slabs
    piece = width // (groups * HALVES)
    span = rows_dev >> second
    long = jnp.left_shift(1, level)
    short = jnp.left_shift(1, second)
    row_ids = jnp.arange(rows_dev, dtype=jnp.int32)
    row_first = here * span + (row_ids >> second)
    row_second = row_ids & short - 1
    edge_ids = jnp.arange(slabs * PLANE, dtype=jnp.int32)
    edge_away = edge_ids // PLANE + 1
    edge_slab = (here + slabs - edge_away) % slabs
    edge_first = edge_slab * span
    edge_second = edge_ids % PLANE
    edge_live = ((edge_away < slabs) & (edge_second < short)).astype(jnp.float32)

    def weights(maker, factor):
        body = maker(row_first[:, None], row_first[None, :], long) * maker(row_second[:, None], row_second[None, :], short)
        edge = maker(row_first[:, None], edge_first[None, :], long) * maker(row_second[:, None], edge_second[None, :], short)
        edge = edge * edge_live[None, :]
        return (factor * jnp.concatenate([body, body, edge, edge], axis=1)).astype(jnp.bfloat16)

    fwd_weights = weights(hier_weight, coeffs[0].astype(jnp.float32))
    back_weights = weights(dehier_weight, 1.0)
    slot_rows = jnp.broadcast_to(slot_map % per_slab, (PLANE, rows_dev))
    f32, bf16 = jnp.float32, jnp.bfloat16
    dma = pltpu.SemaphoreType.DMA
    block = (HALVES, groups, rows_dev, piece)
    in_vmem = pl.BlockSpec(memory_space=pltpu.VMEM)
    result = pl.pallas_call(
        functools.partial(kernel, groups, slabs, per_slab),
        out_shape=jax.ShapeDtypeStruct((rows_dev, width), f32),
        in_specs=[in_vmem] * 4,
        out_specs=in_vmem,
        scratch_shapes=[
            pltpu.VMEM(block, f32),
            pltpu.VMEM(block, f32),
            pltpu.VMEM((per_slab, piece), f32),
            pltpu.VMEM((2 * per_slab, piece), bf16),
            pltpu.VMEM(block, f32),
            pltpu.VMEM(block, f32),
            pltpu.VMEM((slabs, PLANE, width), f32),
            pltpu.VMEM((HALVES, groups, slabs, PLANE, piece), f32),
            pltpu.VMEM((groups, PLANE, rows_dev), jnp.int32),
            pltpu.VMEM((groups, per_slab, 2 * rows_dev), bf16),
            pltpu.VMEM((groups, rows_dev, 2 * per_slab), bf16),
            dma((HALVES, groups, slabs)),
            dma((HALVES, groups, slabs)),
            dma((groups,)),
            dma((groups,)),
            dma((HALVES, groups)),
            dma((HALVES, groups)),
            dma((HALVES, groups)),
            dma((HALVES, groups)),
            dma((HALVES, groups, slabs)),
            dma((HALVES, groups, slabs)),
        ],
        compiler_params=pltpu.CompilerParams(collective_id=0, has_side_effects=True, vmem_limit_bytes=40 << 20),
    )(grid_rows, slot_rows, fwd_weights, back_weights)
    return result[None]


def solution(mesh):
    in_specs = (P("grp", "slab", None), P("grp"), P("grp"), P("grp", "slab"))
    out_specs = P("grp", "slab", None)

    def whole(grids, first_level, coeffs, slot_map):
        groups, rows, width = grids.shape
        few = mesh.shape["grp"] == groups and groups * rows <= 4 * 2 * ROWS
        even = width % (groups * HALVES * LANES) == 0 and rows // mesh.shape["slab"] == LANES
        body = fused_shards if few and even else shards
        step = jax.shard_map(body, mesh=mesh, in_specs=in_specs, out_specs=out_specs, check_vma=False)
        return step(grids, first_level, coeffs, slot_map)

    return whole
```

```python
import functools

import jax
import jax.numpy as jnp
from jax import lax
from jax.experimental import pallas as pl
from jax.experimental.pallas import tpu as pltpu
from jax.sharding import PartitionSpec as P

P2 = 16
P3 = 16
P4 = 16
LEVEL_SUM = 9
PLANE = 8
ROWS = 512
MESH = pl.DeviceIdType.MESH


def hier_weight(target, source, period):
    spread = target & -target
    interior = (target != 0).astype(jnp.float32)
    left_side = (source == target - spread).astype(jnp.float32)
    right_side = (source == (target + spread) % period).astype(jnp.float32)
    return (target == source).astype(jnp.float32) - 0.5 * interior * (left_side + right_side)


def dehier_weight(target, source, period):
    spread = jnp.maximum(source & -source, 1).astype(jnp.float32)
    apart = jnp.abs(target - source)
    apart = jnp.minimum(apart, period - apart).astype(jnp.float32)
    return jnp.where(source == 0, 1.0, jnp.maximum(0.0, 1.0 - apart / spread))


def square_table(maker, length):
    points = jnp.arange(length, dtype=jnp.int32)
    return maker(points[:, None], points[None, :], length)


def inner_apply(values, third_op, rest_op):
    count = values.shape[0]
    shaped = values.reshape(count, P2, P3 * P4)
    shaped = jnp.einsum("ij,rjk->rik", third_op, shaped, precision=lax.Precision.HIGHEST)
    shaped = jnp.einsum("rjk,lk->rjl", shaped, rest_op, precision=lax.Precision.HIGHEST)
    return shaped.reshape(count, P2 * P3 * P4)


def exact_dot(left, right):
    return jnp.dot(left, right, precision=lax.Precision.HIGHEST, preferred_element_type=jnp.float32)


def shards(grids, first_level, coeffs, slot_map):
    grid_rows = grids[0]
    level = first_level[0]
    second = LEVEL_SUM - level
    rows_dev = grid_rows.shape[0]
    width = grid_rows.shape[1]
    slabs = lax.axis_size("slab")
    slab_index = lax.axis_index("slab")
    span = rows_dev >> second
    row_ids = jnp.arange(rows_dev, dtype=jnp.int32)
    first_pos = row_ids >> second
    second_pos = row_ids & (1 << second) - 1
    slab_ids = jnp.arange(slabs, dtype=jnp.int32)
    same_first = (first_pos[:, None] == first_pos[None, :]).astype(jnp.float32)
    hier_third = square_table(hier_weight, P2)
    hier_rest = jnp.kron(square_table(hier_weight, P3), square_table(hier_weight, P4))
    values = inner_apply(grid_rows, hier_third, hier_rest)
    second_op = same_first * hier_weight(second_pos[:, None], second_pos[None, :], 1 << second)
    values = exact_dot(second_op, values)
    plane = values[:PLANE]
    planes = lax.all_gather(plane[None], "slab", axis=0, tiled=True)
    following = lax.dynamic_index_in_dim(planes, (slab_index + 1) % slabs, 0, keepdims=False)
    extended = jnp.concatenate([values, following], axis=0)
    ext_ids = jnp.arange(rows_dev + PLANE, dtype=jnp.int32)
    ext_first = ext_ids >> second
    ext_second = ext_ids & (1 << second) - 1
    spread = first_pos & -first_pos
    interior = (first_pos != 0).astype(jnp.float32)[:, None]
    same_second = (second_pos[:, None] == ext_second[None, :]).astype(jnp.float32)
    centre = (ext_first[None, :] == first_pos[:, None]).astype(jnp.float32)
    below = (ext_first[None, :] == (first_pos - spread)[:, None]).astype(jnp.float32)
    above = (ext_first[None, :] == (first_pos + spread)[:, None]).astype(jnp.float32)
    fine_op = same_second * (centre - 0.5 * interior * (below + above))
    surplus = exact_dot(fine_op, extended)
    coarse_weights = hier_weight(slab_index, slab_ids, slabs)
    coarse = jnp.einsum("q,qpk->pk", coarse_weights, planes, precision=lax.Precision.HIGHEST)
    padded = jnp.concatenate([coarse, jnp.zeros((rows_dev - PLANE, width), jnp.float32)], axis=0)
    surplus = jnp.where((first_pos == 0)[:, None], padded, surplus)
    scaled = coeffs[0].astype(jnp.float32) * surplus
    per_slab = 2 * ROWS // slabs
    slot_local = slot_map[0] % per_slab
    slot_ids = jnp.arange(per_slab, dtype=jnp.int32)
    gather_op = (slot_local[None, :] == slot_ids[:, None]).astype(jnp.float32)
    term = exact_dot(gather_op, scaled)
    total = lax.psum(term, "grp")
    spread_op = (slot_local[:, None] == slot_ids[None, :]).astype(jnp.float32)
    combined = exact_dot(spread_op, total)
    back_third = square_table(dehier_weight, P2)
    back_rest = jnp.kron(square_table(dehier_weight, P3), square_table(dehier_weight, P4))
    values = inner_apply(combined, back_third, back_rest)
    back_second = same_first * dehier_weight(second_pos[:, None], second_pos[None, :], 1 << second)
    values = exact_dot(back_second, values)
    top_plane = values[:PLANE]
    top_planes = lax.all_gather(top_plane[None], "slab", axis=0, tiled=True)
    here_weights = dehier_weight(slab_index, slab_ids, slabs)
    there_weights = dehier_weight((slab_index + 1) % slabs, slab_ids, slabs)
    here = jnp.einsum("q,qpk->pk", here_weights, top_planes, precision=lax.Precision.HIGHEST)
    there = jnp.einsum("q,qpk->pk", there_weights, top_planes, precision=lax.Precision.HIGHEST)
    same_row_second = (second_pos[:, None] == second_pos[None, :]).astype(jnp.float32)
    inside = (first_pos[None, :] != 0).astype(jnp.float32)
    local_op = (
        same_row_second * inside * dehier_weight(first_pos[:, None], first_pos[None, :], 2 * span)
    )
    fraction = first_pos.astype(jnp.float32) / span.astype(jnp.float32)
    plane_ids = jnp.arange(PLANE, dtype=jnp.int32)
    plane_pick = (second_pos[:, None] == plane_ids[None, :]).astype(jnp.float32)
    nodal = exact_dot(local_op, values)
    nodal = nodal + exact_dot((1.0 - fraction)[:, None] * plane_pick, here)
    nodal = nodal + exact_dot(fraction[:, None] * plane_pick, there)
    return nodal[None]


PAIR = 2
LANES = 128
PACK = 4
LAG = 2
HOP = 2


def split_pair(values):
    high = values.astype(jnp.bfloat16)
    low = (values - high.astype(jnp.float32)).astype(jnp.bfloat16)
    return high, low


def mix(weights, body, edge):
    body_high, body_low = split_pair(body)
    edge_high, edge_low = split_pair(edge)
    stacked = jnp.concatenate([body_high, body_low, edge_high, edge_low], axis=0)
    return jnp.dot(weights, stacked, preferred_element_type=jnp.float32)


def kernel(groups, slabs, per_slab, grid_ref, slot_ref, fwd_ref, back_ref, out_ref,
           mine, sent, got, own, pre, suf, pre_out, suf_out, back, vals, planes, tops, slots, pick, place,
           plane_send, plane_recv, slot_sems, y_send, y_recv, pre_send, pre_recv, suf_send, suf_recv,
           back_send, back_recv, top_send, top_recv):
    me = lax.axis_index("grp")
    here = lax.axis_index("slab")
    rows, width = grid_ref.shape
    chunks = own.shape[0]
    piece = own.shape[2]
    side = lax.rem(me, PAIR)
    line = me // PAIR
    length = groups // PAIR
    partner = me + 1 - 2 * side
    right = lax.rem(me + PAIR, groups)
    left = lax.rem(me + groups - PAIR, groups)
    half = width // PAIR

    def slab_at(step):
        return lax.rem(here + step, slabs)

    def columns(other, chunk):
        base = (side if other == 0 else 1 - side) * half
        return pl.ds(pl.multiple_of(base + chunk * piece, piece), piece)

    def remote(src, dst, send, recv, axis, target):
        return pltpu.make_async_remote_copy(
            src_ref=src, dst_ref=dst, send_sem=send, recv_sem=recv,
            device_id={axis: target}, device_id_type=MESH,
        )

    barrier = pltpu.get_barrier_semaphore()
    for target in (partner, left, right):
        pl.semaphore_signal(barrier, inc=1, device_id={"grp": target}, device_id_type=MESH)
    for step in range(1, slabs):
        pl.semaphore_signal(barrier, inc=1, device_id={"slab": slab_at(step)}, device_id_type=MESH)
    pl.semaphore_wait(barrier, slabs + 2)

    packs = chunks // PACK

    def plane_copy(other, pack, away):
        base = (side if other == 0 else 1 - side) * half
        cols = pl.ds(pl.multiple_of(base + pack * PACK * piece, piece), PACK * piece)
        return remote(grid_ref.at[pl.ds(0, PLANE), cols], planes.at[away, :, cols],
                      plane_send.at[other, pack, away], plane_recv.at[other, pack, away], "slab", slab_at(away))

    def y_copy(c):
        return remote(sent.at[c], got.at[c], y_send.at[c], y_recv.at[c], "grp", partner)

    def pre_copy(c):
        return remote(pre_out.at[c], pre.at[c], pre_send.at[c], pre_recv.at[c], "grp", right)

    def suf_copy(c):
        return remote(suf_out.at[c], suf.at[c], suf_send.at[c], suf_recv.at[c], "grp", left)

    def back_copy(c):
        return remote(back.at[c], vals.at[1, c], back_send.at[c], back_recv.at[c], "grp", partner)

    def top_copy(other, c, away):
        return remote(vals.at[other, c, pl.ds(0, PLANE), :], tops.at[other, c, away],
                      top_send.at[other, c, away], top_recv.at[other, c, away], "slab", slab_at(away))

    slot_copy = remote(slot_ref, slots, slot_sems.at[0], slot_sems.at[1], "grp", partner)

    for pack in range(packs):
        for other in (1, 0):
            for away in range(1, slabs):
                plane_copy(other, pack, away).start()
        if pack == 0:
            slot_copy.start()

    @pl.when(line == 0)
    def _():
        pre[...] = jnp.zeros_like(pre)

    @pl.when(line == length - 1)
    def _():
        suf[...] = jnp.zeros_like(suf)

    slot_ids = lax.broadcasted_iota(jnp.int32, (per_slab, rows), 0)

    def fill(index, row_slots):
        hit = jnp.where(slot_ids == row_slots, 1.0, 0.0)
        flat = hit.astype(jnp.bfloat16)
        pick[index] = jnp.concatenate([flat, flat], axis=1)
        turned = jnp.transpose(hit).astype(jnp.bfloat16)
        place[index] = jnp.concatenate([turned, turned], axis=1)

    fill(0, slot_ref[0:1, :])

    def scaled(other, c):
        cols = columns(other, c)
        edge = [planes[away, :, cols] for away in range(1, slabs)]
        edge.append(jnp.zeros((PLANE, piece), jnp.float32))
        return mix(fwd_ref[...], grid_ref[:, cols], jnp.concatenate(edge, axis=0))

    def at(c, body):
        pl.when((c >= 0) & (c < chunks))(lambda: body(c))

    def start(c):
        @pl.when(lax.rem(c, PACK) == 0)
        def _():
            for other in (1, 0):
                for away in range(1, slabs):
                    plane_copy(other, c // PACK, away).wait_recv()

        sent[c] = scaled(1, c)
        y_copy(c).start()
        mine[c] = scaled(0, c)

    def merge(c):
        high, low = split_pair(mine[c])
        first = jnp.dot(pick[0], jnp.concatenate([high, low], axis=0), preferred_element_type=jnp.float32)
        y_copy(c).wait_recv()
        high, low = split_pair(got[c])
        own[c] = first + jnp.dot(pick[1], jnp.concatenate([high, low], axis=0), preferred_element_type=jnp.float32)

    def from_left(c):
        @pl.when(line > 0)
        def _():
            pre_copy(c).wait_recv()

        @pl.when(line < length - 1)
        def _():
            pre_out[c] = pre[c] + own[c]
            pre_copy(c).start()

    def from_right(c):
        @pl.when(line < length - 1)
        def _():
            suf_copy(c).wait_recv()

        @pl.when(line > 0)
        def _():
            suf_out[c] = suf[c] + own[c]
            suf_copy(c).start()

    def rebuild(c):
        high, low = split_pair(pre[c] + own[c] + suf[c])
        both = jnp.concatenate([high, low], axis=0)
        back[c] = jnp.dot(place[1], both, preferred_element_type=jnp.float32)
        back_copy(c).start()
        vals[0, c] = jnp.dot(place[0], both, preferred_element_type=jnp.float32)

    def share(c):
        for away in range(1, slabs):
            top_copy(0, c, away).start()
        back_copy(c).wait_recv()
        for away in range(1, slabs):
            top_copy(1, c, away).start()

    def finish(c):
        for other in range(2):
            for away in range(1, slabs):
                top_copy(other, c, away).wait_recv()
            edge = [tops[other, c, away] for away in range(1, slabs)]
            edge.append(jnp.zeros((PLANE, piece), jnp.float32))
            out_ref[:, columns(other, c)] = mix(back_ref[...], vals[other, c], jnp.concatenate(edge, axis=0))

    def round_of(t, carry):
        at(t, start)

        @pl.when(t == 0)
        def _():
            slot_copy.wait_recv()
            fill(1, slots[0:1, :])

        ready = t - LAG
        at(ready, merge)
        at(ready - HOP * line, from_left)
        at(ready - HOP * (length - 1 - line), from_right)
        done = ready - HOP * jnp.maximum(line, length - 1 - line)
        at(done, rebuild)
        at(done - LAG, share)
        at(done - LAG - 1, finish)
        return carry

    lax.fori_loop(0, chunks + 2 * LAG + 1 + HOP * (length - 1), round_of, 0)

    def drain(c, carry):
        y_copy(c).wait_send()
        back_copy(c).wait_send()

        @pl.when(line < length - 1)
        def _():
            pre_copy(c).wait_send()

        @pl.when(line > 0)
        def _():
            suf_copy(c).wait_send()

        for other in range(2):
            for away in range(1, slabs):
                top_copy(other, c, away).wait_send()
        return carry

    lax.fori_loop(0, chunks, drain, 0)
    for pack in range(packs):
        for other in range(2):
            for away in range(1, slabs):
                plane_copy(other, pack, away).wait_send()
    slot_copy.wait_send()


def fused_shards(grids, first_level, coeffs, slot_map):
    grid_rows = grids[0]
    level = first_level[0]
    second = LEVEL_SUM - level
    rows_dev, width = grid_rows.shape
    slabs = lax.axis_size("slab")
    groups = lax.axis_size("grp")
    here = lax.axis_index("slab")
    per_slab = 2 * ROWS // slabs
    piece = LANES
    chunks = width // (PAIR * piece)
    span = rows_dev >> second
    long = jnp.left_shift(1, level)
    short = jnp.left_shift(1, second)
    row_ids = jnp.arange(rows_dev, dtype=jnp.int32)
    row_first = here * span + (row_ids >> second)
    row_second = row_ids & short - 1
    edge_ids = jnp.arange(slabs * PLANE, dtype=jnp.int32)
    edge_away = edge_ids // PLANE + 1
    edge_slab = (here + slabs - edge_away) % slabs
    edge_first = edge_slab * span
    edge_second = edge_ids % PLANE
    edge_live = ((edge_away < slabs) & (edge_second < short)).astype(jnp.float32)

    def weights(maker, factor):
        body = maker(row_first[:, None], row_first[None, :], long) * maker(row_second[:, None], row_second[None, :], short)
        edge = maker(row_first[:, None], edge_first[None, :], long) * maker(row_second[:, None], edge_second[None, :], short)
        edge = edge * edge_live[None, :]
        return (factor * jnp.concatenate([body, body, edge, edge], axis=1)).astype(jnp.bfloat16)

    fwd_weights = weights(hier_weight, coeffs[0].astype(jnp.float32))
    back_weights = weights(dehier_weight, 1.0)
    slot_rows = jnp.broadcast_to(slot_map % per_slab, (PLANE, rows_dev))
    f32, bf16 = jnp.float32, jnp.bfloat16
    dma = pltpu.SemaphoreType.DMA
    short_block = (chunks, rows_dev, piece)
    tall_block = (chunks, per_slab, piece)
    in_vmem = pl.BlockSpec(memory_space=pltpu.VMEM)
    result = pl.pallas_call(
        functools.partial(kernel, groups, slabs, per_slab),
        out_shape=jax.ShapeDtypeStruct((rows_dev, width), f32),
        in_specs=[in_vmem] * 4,
        out_specs=in_vmem,
        scratch_shapes=[
            pltpu.VMEM(short_block, f32),
            pltpu.VMEM(short_block, f32),
            pltpu.VMEM(short_block, f32),
            pltpu.VMEM(tall_block, f32),
            pltpu.VMEM(tall_block, f32),
            pltpu.VMEM(tall_block, f32),
            pltpu.VMEM(tall_block, f32),
            pltpu.VMEM(tall_block, f32),
            pltpu.VMEM(short_block, f32),
            pltpu.VMEM((2,) + short_block, f32),
            pltpu.VMEM((slabs, PLANE, width), f32),
            pltpu.VMEM((2, chunks, slabs, PLANE, piece), f32),
            pltpu.VMEM((PLANE, rows_dev), jnp.int32),
            pltpu.VMEM((2, per_slab, 2 * rows_dev), bf16),
            pltpu.VMEM((2, rows_dev, 2 * per_slab), bf16),
            dma((2, chunks // PACK, slabs)),
            dma((2, chunks // PACK, slabs)),
            dma((2,)),
            dma((chunks,)),
            dma((chunks,)),
            dma((chunks,)),
            dma((chunks,)),
            dma((chunks,)),
            dma((chunks,)),
            dma((chunks,)),
            dma((chunks,)),
            dma((2, chunks, slabs)),
            dma((2, chunks, slabs)),
        ],
        compiler_params=pltpu.CompilerParams(collective_id=0, has_side_effects=True, vmem_limit_bytes=40 << 20),
    )(grid_rows, slot_rows, fwd_weights, back_weights)
    return result[None]


def solution(mesh):
    in_specs = (P("grp", "slab", None), P("grp"), P("grp"), P("grp", "slab"))
    out_specs = P("grp", "slab", None)

    def whole(grids, first_level, coeffs, slot_map):
        groups, rows, width = grids.shape
        few = mesh.shape["grp"] == groups and groups * rows <= 4 * 2 * ROWS
        even = groups % PAIR == 0 and groups > PAIR and width % (PAIR * PACK * LANES) == 0 and rows // mesh.shape["slab"] == LANES
        body = fused_shards if few and even else shards
        step = jax.shard_map(body, mesh=mesh, in_specs=in_specs, out_specs=out_specs, check_vma=False)
        return step(grids, first_level, coeffs, slot_map)

    return whole
```

```python
import functools

import jax
import jax.numpy as jnp
from jax import lax
from jax.experimental import pallas as pl
from jax.experimental.pallas import tpu as pltpu
from jax.sharding import PartitionSpec as P

P2 = 16
P3 = 16
P4 = 16
LEVEL_SUM = 9
PLANE = 8
ROWS = 512
MESH = pl.DeviceIdType.MESH


def hier_weight(target, source, period):
    spread = target & -target
    interior = (target != 0).astype(jnp.float32)
    left_side = (source == target - spread).astype(jnp.float32)
    right_side = (source == (target + spread) % period).astype(jnp.float32)
    return (target == source).astype(jnp.float32) - 0.5 * interior * (left_side + right_side)


def dehier_weight(target, source, period):
    spread = jnp.maximum(source & -source, 1).astype(jnp.float32)
    apart = jnp.abs(target - source)
    apart = jnp.minimum(apart, period - apart).astype(jnp.float32)
    return jnp.where(source == 0, 1.0, jnp.maximum(0.0, 1.0 - apart / spread))


def square_table(maker, length):
    points = jnp.arange(length, dtype=jnp.int32)
    return maker(points[:, None], points[None, :], length)


def inner_apply(values, third_op, rest_op):
    count = values.shape[0]
    shaped = values.reshape(count, P2, P3 * P4)
    shaped = jnp.einsum("ij,rjk->rik", third_op, shaped, precision=lax.Precision.HIGHEST)
    shaped = jnp.einsum("rjk,lk->rjl", shaped, rest_op, precision=lax.Precision.HIGHEST)
    return shaped.reshape(count, P2 * P3 * P4)


def exact_dot(left, right):
    return jnp.dot(left, right, precision=lax.Precision.HIGHEST, preferred_element_type=jnp.float32)


def shards(grids, first_level, coeffs, slot_map):
    grid_rows = grids[0]
    level = first_level[0]
    second = LEVEL_SUM - level
    rows_dev = grid_rows.shape[0]
    width = grid_rows.shape[1]
    slabs = lax.axis_size("slab")
    slab_index = lax.axis_index("slab")
    span = rows_dev >> second
    row_ids = jnp.arange(rows_dev, dtype=jnp.int32)
    first_pos = row_ids >> second
    second_pos = row_ids & (1 << second) - 1
    slab_ids = jnp.arange(slabs, dtype=jnp.int32)
    same_first = (first_pos[:, None] == first_pos[None, :]).astype(jnp.float32)
    hier_third = square_table(hier_weight, P2)
    hier_rest = jnp.kron(square_table(hier_weight, P3), square_table(hier_weight, P4))
    values = inner_apply(grid_rows, hier_third, hier_rest)
    second_op = same_first * hier_weight(second_pos[:, None], second_pos[None, :], 1 << second)
    values = exact_dot(second_op, values)
    plane = values[:PLANE]
    planes = lax.all_gather(plane[None], "slab", axis=0, tiled=True)
    following = lax.dynamic_index_in_dim(planes, (slab_index + 1) % slabs, 0, keepdims=False)
    extended = jnp.concatenate([values, following], axis=0)
    ext_ids = jnp.arange(rows_dev + PLANE, dtype=jnp.int32)
    ext_first = ext_ids >> second
    ext_second = ext_ids & (1 << second) - 1
    spread = first_pos & -first_pos
    interior = (first_pos != 0).astype(jnp.float32)[:, None]
    same_second = (second_pos[:, None] == ext_second[None, :]).astype(jnp.float32)
    centre = (ext_first[None, :] == first_pos[:, None]).astype(jnp.float32)
    below = (ext_first[None, :] == (first_pos - spread)[:, None]).astype(jnp.float32)
    above = (ext_first[None, :] == (first_pos + spread)[:, None]).astype(jnp.float32)
    fine_op = same_second * (centre - 0.5 * interior * (below + above))
    surplus = exact_dot(fine_op, extended)
    coarse_weights = hier_weight(slab_index, slab_ids, slabs)
    coarse = jnp.einsum("q,qpk->pk", coarse_weights, planes, precision=lax.Precision.HIGHEST)
    padded = jnp.concatenate([coarse, jnp.zeros((rows_dev - PLANE, width), jnp.float32)], axis=0)
    surplus = jnp.where((first_pos == 0)[:, None], padded, surplus)
    scaled = coeffs[0].astype(jnp.float32) * surplus
    per_slab = 2 * ROWS // slabs
    slot_local = slot_map[0] % per_slab
    slot_ids = jnp.arange(per_slab, dtype=jnp.int32)
    gather_op = (slot_local[None, :] == slot_ids[:, None]).astype(jnp.float32)
    term = exact_dot(gather_op, scaled)
    total = lax.psum(term, "grp")
    spread_op = (slot_local[:, None] == slot_ids[None, :]).astype(jnp.float32)
    combined = exact_dot(spread_op, total)
    back_third = square_table(dehier_weight, P2)
    back_rest = jnp.kron(square_table(dehier_weight, P3), square_table(dehier_weight, P4))
    values = inner_apply(combined, back_third, back_rest)
    back_second = same_first * dehier_weight(second_pos[:, None], second_pos[None, :], 1 << second)
    values = exact_dot(back_second, values)
    top_plane = values[:PLANE]
    top_planes = lax.all_gather(top_plane[None], "slab", axis=0, tiled=True)
    here_weights = dehier_weight(slab_index, slab_ids, slabs)
    there_weights = dehier_weight((slab_index + 1) % slabs, slab_ids, slabs)
    here = jnp.einsum("q,qpk->pk", here_weights, top_planes, precision=lax.Precision.HIGHEST)
    there = jnp.einsum("q,qpk->pk", there_weights, top_planes, precision=lax.Precision.HIGHEST)
    same_row_second = (second_pos[:, None] == second_pos[None, :]).astype(jnp.float32)
    inside = (first_pos[None, :] != 0).astype(jnp.float32)
    local_op = (
        same_row_second * inside * dehier_weight(first_pos[:, None], first_pos[None, :], 2 * span)
    )
    fraction = first_pos.astype(jnp.float32) / span.astype(jnp.float32)
    plane_ids = jnp.arange(PLANE, dtype=jnp.int32)
    plane_pick = (second_pos[:, None] == plane_ids[None, :]).astype(jnp.float32)
    nodal = exact_dot(local_op, values)
    nodal = nodal + exact_dot((1.0 - fraction)[:, None] * plane_pick, here)
    nodal = nodal + exact_dot(fraction[:, None] * plane_pick, there)
    return nodal[None]


PAIR = 2
LANES = 128
PACK = 4
LAG = 2
HOP = 2
PARTS = 2


def split_pair(values):
    high = values.astype(jnp.bfloat16)
    low = (values - high.astype(jnp.float32)).astype(jnp.bfloat16)
    return high, low


def mix(weights, body, edge):
    body_high, body_low = split_pair(body)
    edge_high, edge_low = split_pair(edge)
    stacked = jnp.concatenate([body_high, body_low, edge_high, edge_low], axis=0)
    return jnp.dot(weights, stacked, preferred_element_type=jnp.float32)


def kernel(groups, slabs, per_slab, grid_ref, slot_ref, fwd_ref, back_ref, out_ref,
           mine, sent, got, own, pre, suf, pre_out, suf_out, back, vals, planes, tops, slots, pick, place,
           plane_send, plane_recv, slot_sems, y_send, y_recv, pre_send, pre_recv, suf_send, suf_recv,
           back_send, back_recv, top_send, top_recv):
    me = lax.axis_index("grp")
    here = lax.axis_index("slab")
    rows, width = grid_ref.shape
    chunks = own.shape[0]
    piece = own.shape[2]
    side = lax.rem(me, PAIR)
    line = me // PAIR
    length = groups // PAIR
    partner = me + 1 - 2 * side
    right = lax.rem(me + PAIR, groups)
    left = lax.rem(me + groups - PAIR, groups)
    half = width // PAIR

    def slab_at(step):
        return lax.rem(here + step, slabs)

    def columns(other, chunk):
        base = (side if other == 0 else 1 - side) * half
        return pl.ds(pl.multiple_of(base + chunk * piece, piece), piece)

    def remote(src, dst, send, recv, axis, target):
        return pltpu.make_async_remote_copy(
            src_ref=src, dst_ref=dst, send_sem=send, recv_sem=recv,
            device_id={axis: target}, device_id_type=MESH,
        )

    barrier = pltpu.get_barrier_semaphore()
    for target in (partner, left, right):
        pl.semaphore_signal(barrier, inc=1, device_id={"grp": target}, device_id_type=MESH)
    for step in range(1, slabs):
        pl.semaphore_signal(barrier, inc=1, device_id={"slab": slab_at(step)}, device_id_type=MESH)
    pl.semaphore_wait(barrier, slabs + 2)

    packs = chunks // PACK

    def plane_copy(other, pack, away):
        base = (side if other == 0 else 1 - side) * half
        cols = pl.ds(pl.multiple_of(base + pack * PACK * piece, piece), PACK * piece)
        return remote(grid_ref.at[pl.ds(0, PLANE), cols], planes.at[away, :, cols],
                      plane_send.at[other, pack, away], plane_recv.at[other, pack, away], "slab", slab_at(away))

    def y_copy(c):
        return remote(sent.at[c], got.at[c], y_send.at[c], y_recv.at[c], "grp", partner)

    def share_of(part):
        return pl.ds(part * (per_slab // PARTS), per_slab // PARTS)

    def pre_copy(c, part):
        return remote(pre_out.at[c, share_of(part)], pre.at[c, share_of(part)],
                      pre_send.at[c, part], pre_recv.at[c, part], "grp", right)

    def suf_copy(c, part):
        return remote(suf_out.at[c, share_of(part)], suf.at[c, share_of(part)],
                      suf_send.at[c, part], suf_recv.at[c, part], "grp", left)

    def back_copy(c):
        return remote(back.at[c], vals.at[1, c], back_send.at[c], back_recv.at[c], "grp", partner)

    def top_copy(other, c, away):
        return remote(vals.at[other, c, pl.ds(0, PLANE), :], tops.at[other, c, away],
                      top_send.at[other, c, away], top_recv.at[other, c, away], "slab", slab_at(away))

    slot_copy = remote(slot_ref, slots, slot_sems.at[0], slot_sems.at[1], "grp", partner)

    for pack in range(packs):
        for other in (1, 0):
            for away in range(1, slabs):
                plane_copy(other, pack, away).start()
        if pack == 0:
            slot_copy.start()

    @pl.when(line == 0)
    def _():
        pre[...] = jnp.zeros_like(pre)

    @pl.when(line == length - 1)
    def _():
        suf[...] = jnp.zeros_like(suf)

    slot_ids = lax.broadcasted_iota(jnp.int32, (per_slab, rows), 0)

    def fill(index, row_slots):
        hit = jnp.where(slot_ids == row_slots, 1.0, 0.0)
        flat = hit.astype(jnp.bfloat16)
        for copy in range(2):
            pick[:, pl.ds((2 * copy + index) * rows, rows)] = flat
        turned = jnp.transpose(hit).astype(jnp.bfloat16)
        place[pl.ds(index * rows, rows), :] = jnp.concatenate([turned, turned], axis=1)

    fill(0, slot_ref[0:1, :])

    def edges(parts):
        return jnp.concatenate(parts + [jnp.zeros((PLANE, piece), jnp.float32)], axis=0)

    def at(c, body):
        pl.when((c >= 0) & (c < chunks))(lambda: body(c))

    def start(c):
        @pl.when(lax.rem(c, PACK) == 0)
        def _():
            for other in (1, 0):
                for away in range(1, slabs):
                    plane_copy(other, c // PACK, away).wait_recv()

        both = [columns(1, c), columns(0, c)]
        body = jnp.concatenate([grid_ref[:, cols] for cols in both], axis=1)
        edge = [edges([planes[away, :, cols] for away in range(1, slabs)]) for cols in both]
        scaled = mix(fwd_ref[...], body, jnp.concatenate(edge, axis=1))
        sent[c] = scaled[:, :piece]
        y_copy(c).start()
        mine[c] = scaled[:, piece:]

    def merge(c):
        y_copy(c).wait_recv()
        high, low = split_pair(jnp.concatenate([mine[c], got[c]], axis=0))
        own[c] = jnp.dot(pick[...], jnp.concatenate([high, low], axis=0), preferred_element_type=jnp.float32)

    def from_left(c):
        for part in range(PARTS):
            @pl.when(line > 0)
            def _():
                pre_copy(c, part).wait_recv()

            @pl.when(line < length - 1)
            def _():
                pre_out[c, share_of(part)] = pre[c, share_of(part)] + own[c, share_of(part)]
                pre_copy(c, part).start()

    def from_right(c):
        for part in range(PARTS):
            @pl.when(line < length - 1)
            def _():
                suf_copy(c, part).wait_recv()

            @pl.when(line > 0)
            def _():
                suf_out[c, share_of(part)] = suf[c, share_of(part)] + own[c, share_of(part)]
                suf_copy(c, part).start()

    def rebuild(c):
        high, low = split_pair(pre[c] + own[c] + suf[c])
        both = jnp.concatenate([high, low], axis=0)
        placed = jnp.dot(place[...], both, preferred_element_type=jnp.float32)
        back[c] = placed[rows:]
        back_copy(c).start()
        vals[0, c] = placed[:rows]

    def share(c):
        for away in range(1, slabs):
            top_copy(0, c, away).start()
        back_copy(c).wait_recv()
        for away in range(1, slabs):
            top_copy(1, c, away).start()

    def finish(c):
        edge = []
        for other in range(2):
            for away in range(1, slabs):
                top_copy(other, c, away).wait_recv()
            edge.append(edges([tops[other, c, away] for away in range(1, slabs)]))
        body = jnp.concatenate([vals[0, c], vals[1, c]], axis=1)
        nodal = mix(back_ref[...], body, jnp.concatenate(edge, axis=1))
        out_ref[:, columns(0, c)] = nodal[:, :piece]
        out_ref[:, columns(1, c)] = nodal[:, piece:]

    def round_of(t, carry):
        at(t, start)

        @pl.when(t == 0)
        def _():
            slot_copy.wait_recv()
            fill(1, slots[0:1, :])

        ready = t - LAG
        at(ready, merge)
        at(ready - HOP * line, from_left)
        at(ready - HOP * (length - 1 - line), from_right)
        done = ready - HOP * jnp.maximum(line, length - 1 - line)
        at(done, rebuild)
        at(done - LAG, share)
        at(done - LAG - 1, finish)
        return carry

    lax.fori_loop(0, chunks + 2 * LAG + 1 + HOP * (length - 1), round_of, 0)

    def drain(c, carry):
        y_copy(c).wait_send()
        back_copy(c).wait_send()

        @pl.when(line < length - 1)
        def _():
            for part in range(PARTS):
                pre_copy(c, part).wait_send()

        @pl.when(line > 0)
        def _():
            for part in range(PARTS):
                suf_copy(c, part).wait_send()

        for other in range(2):
            for away in range(1, slabs):
                top_copy(other, c, away).wait_send()
        return carry

    lax.fori_loop(0, chunks, drain, 0)
    for pack in range(packs):
        for other in range(2):
            for away in range(1, slabs):
                plane_copy(other, pack, away).wait_send()
    slot_copy.wait_send()


def fused_shards(grids, first_level, coeffs, slot_map):
    grid_rows = grids[0]
    level = first_level[0]
    second = LEVEL_SUM - level
    rows_dev, width = grid_rows.shape
    slabs = lax.axis_size("slab")
    groups = lax.axis_size("grp")
    here = lax.axis_index("slab")
    per_slab = 2 * ROWS // slabs
    piece = LANES
    chunks = width // (PAIR * piece)
    span = rows_dev >> second
    long = jnp.left_shift(1, level)
    short = jnp.left_shift(1, second)
    row_ids = jnp.arange(rows_dev, dtype=jnp.int32)
    row_first = here * span + (row_ids >> second)
    row_second = row_ids & short - 1
    edge_ids = jnp.arange(slabs * PLANE, dtype=jnp.int32)
    edge_away = edge_ids // PLANE + 1
    edge_slab = (here + slabs - edge_away) % slabs
    edge_first = edge_slab * span
    edge_second = edge_ids % PLANE
    edge_live = ((edge_away < slabs) & (edge_second < short)).astype(jnp.float32)

    def weights(maker, factor):
        body = maker(row_first[:, None], row_first[None, :], long) * maker(row_second[:, None], row_second[None, :], short)
        edge = maker(row_first[:, None], edge_first[None, :], long) * maker(row_second[:, None], edge_second[None, :], short)
        edge = edge * edge_live[None, :]
        return (factor * jnp.concatenate([body, body, edge, edge], axis=1)).astype(jnp.bfloat16)

    fwd_weights = weights(hier_weight, coeffs[0].astype(jnp.float32))
    back_weights = weights(dehier_weight, 1.0)
    slot_rows = jnp.broadcast_to(slot_map % per_slab, (PLANE, rows_dev))
    f32, bf16 = jnp.float32, jnp.bfloat16
    dma = pltpu.SemaphoreType.DMA
    short_block = (chunks, rows_dev, piece)
    tall_block = (chunks, per_slab, piece)
    in_vmem = pl.BlockSpec(memory_space=pltpu.VMEM)
    result = pl.pallas_call(
        functools.partial(kernel, groups, slabs, per_slab),
        out_shape=jax.ShapeDtypeStruct((rows_dev, width), f32),
        in_specs=[in_vmem] * 4,
        out_specs=in_vmem,
        scratch_shapes=[
            pltpu.VMEM(short_block, f32),
            pltpu.VMEM(short_block, f32),
            pltpu.VMEM(short_block, f32),
            pltpu.VMEM(tall_block, f32),
            pltpu.VMEM(tall_block, f32),
            pltpu.VMEM(tall_block, f32),
            pltpu.VMEM(tall_block, f32),
            pltpu.VMEM(tall_block, f32),
            pltpu.VMEM(short_block, f32),
            pltpu.VMEM((2,) + short_block, f32),
            pltpu.VMEM((slabs, PLANE, width), f32),
            pltpu.VMEM((2, chunks, slabs, PLANE, piece), f32),
            pltpu.VMEM((PLANE, rows_dev), jnp.int32),
            pltpu.VMEM((per_slab, 4 * rows_dev), bf16),
            pltpu.VMEM((2 * rows_dev, 2 * per_slab), bf16),
            dma((2, chunks // PACK, slabs)),
            dma((2, chunks // PACK, slabs)),
            dma((2,)),
            dma((chunks,)),
            dma((chunks,)),
            dma((chunks, PARTS)),
            dma((chunks, PARTS)),
            dma((chunks, PARTS)),
            dma((chunks, PARTS)),
            dma((chunks,)),
            dma((chunks,)),
            dma((2, chunks, slabs)),
            dma((2, chunks, slabs)),
        ],
        compiler_params=pltpu.CompilerParams(collective_id=0, has_side_effects=True, vmem_limit_bytes=40 << 20),
    )(grid_rows, slot_rows, fwd_weights, back_weights)
    return result[None]


def solution(mesh):
    in_specs = (P("grp", "slab", None), P("grp"), P("grp"), P("grp", "slab"))
    out_specs = P("grp", "slab", None)

    def whole(grids, first_level, coeffs, slot_map):
        groups, rows, width = grids.shape
        few = mesh.shape["grp"] == groups and groups * rows <= 4 * 2 * ROWS
        even = groups % PAIR == 0 and groups > PAIR and width % (PAIR * PACK * LANES) == 0 and rows // mesh.shape["slab"] == LANES
        body = fused_shards if few and even else shards
        step = jax.shard_map(body, mesh=mesh, in_specs=in_specs, out_specs=out_specs, check_vma=False)
        return step(grids, first_level, coeffs, slot_map)

    return whole
```
